128 devices in a mesh: dp: 8 (over x, core), crop: 4 (over y), tensor: 4 (over z).
Axes of the slice: x: 4, y: 4, z: 4, core: 2. Of those that a mesh axis runs over, the one named last changes fastest.
Arguments:
- hidden_a: bfloat16 [2048, 8192], P('crop', 'dp'), as said below
- hidden_b: bfloat16 [2048, 8192], P('crop', 'dp'), as said below
- weight: bfloat16 [8192, 8192], P('dp', 'tensor')
Outputs:
- weight_grad: float32 [8192, 8192], P(('dp', 'crop'), 'tensor')
Inputs may be any that keep to these rules, and one draw needn't show every extreme that they name: `hidden_a`: nonnegative entries. `hidden_b`: nonnegative entries.
All inputs are finite; a program needn't handle non-finite values.
Results may differ from the reference program's by a relative error of at most 0.0015.
Values may be sent and summed in bfloat16 or wider, within the bound.
No kernel may reach another device: no remote copies, remote signals or barrier semaphores. Data moves between devices by JAX's collectives and lax.ppermute only.
A program may use at most 128 MiB of HBM per device.

```python
import jax
import jax.numpy as jnp
from jax import lax

H = 8192
F = 8192
B = 2048


def rising_scale(low, high, count):
    position = jnp.arange(count, dtype=jnp.float32) / jnp.float32(max(count - 1, 1))
    level = jnp.exp(jnp.log(jnp.float32(low)) + position * (jnp.log(jnp.float32(high)) - jnp.log(jnp.float32(low))))
    return level / jnp.sqrt(jnp.mean(level * level))


def hidden_pair(key):
    shared = jnp.clip(jax.random.normal(jax.random.fold_in(key, 21), (B, H), jnp.float32), -6.0, 6.0)
    left_noise = jnp.clip(jax.random.normal(jax.random.fold_in(key, 22), (B, H), jnp.float32), -6.0, 6.0)
    right_noise = jnp.clip(jax.random.normal(jax.random.fold_in(key, 23), (B, H), jnp.float32), -6.0, 6.0)
    row_scale = rising_scale(0.5, 2.5, B)[:, None]
    left = jnp.maximum(shared + 0.6 * left_noise, 0.0) * row_scale
    right = jnp.maximum(shared + 0.6 * right_noise, 0.0) * row_scale
    return (left, right)


def draw_hidden_a(key, part):
    return hidden_pair(key)[0].astype(jnp.bfloat16)


def draw_hidden_b(key, part):
    return hidden_pair(key)[1].astype(jnp.bfloat16)


def draw_weight(key, part):
    base_key = jax.random.fold_in(key, 11)
    band_key = jax.random.fold_in(key, 12)
    level_key = jax.random.fold_in(key, 13)
    base = jnp.clip(jax.random.normal(base_key, (H, F), jnp.float32), -6.0, 6.0) / jnp.sqrt(jnp.float32(H))
    upper = jax.random.bernoulli(band_key, 0.5, (F,))
    level = jax.random.uniform(level_key, (F,), jnp.float32)
    low_scale = jnp.exp(jnp.log(0.4) + level * (jnp.log(0.9) - jnp.log(0.4)))
    high_scale = jnp.exp(jnp.log(2.4) + level * (jnp.log(3.6) - jnp.log(2.4)))
    column_scale = jnp.where(upper, high_scale, low_scale)
    return (base * column_scale[None, :]).astype(jnp.bfloat16)


def setup_inputs(seed: int = 0) -> dict:
    key_of = jax.random.split(jax.random.key(seed), 4)
    hidden_a = draw_hidden_a(jax.random.fold_in(key_of[3], 71), 0)
    hidden_b = draw_hidden_b(jax.random.fold_in(key_of[3], 71), 0)
    weight = draw_weight(jax.random.fold_in(key_of[3], 71), 0)
    return dict(hidden_a=hidden_a, hidden_b=hidden_b, weight=weight)


epsilon = 0.0001

def reference(hidden_a, hidden_b, weight):
    total_rows = hidden_a.shape[0]
    left_proj = jnp.dot(hidden_a, weight, preferred_element_type=jnp.float32).astype(jnp.bfloat16)
    right_proj = jnp.dot(hidden_b, weight, preferred_element_type=jnp.float32).astype(jnp.bfloat16)
    stacked = jnp.stack([left_proj, right_proj]).astype(jnp.float32)
    col_means = lax.optimization_barrier(jnp.mean(stacked, axis=1))
    centered = stacked - col_means[:, None, :]
    spread = lax.optimization_barrier(jnp.sum(centered * centered, axis=1))
    deviation = jnp.sqrt(spread / (total_rows - 1.0) + epsilon)
    rounded = centered.astype(jnp.bfloat16)
    products = []
    for branch in range(2):
        gram_full = lax.dot_general(rounded[branch], rounded[branch], (((1,), (1,)), ((), ())), preferred_element_type=jnp.float32)
        products.append(jnp.dot(gram_full.astype(jnp.bfloat16), rounded[branch], preferred_element_type=jnp.float32))
    products = jnp.stack(products)
    hinge_rate = jnp.where(deviation < 1.0, 25.0 / ((total_rows - 1.0) * deviation), 0.0)[:, None, :]
    differ = stacked[0] - stacked[1]
    pull_term = jnp.stack([differ, -differ]) * (50.0 / total_rows)
    cov_scale = 4.0 / (total_rows - 1.0) ** 2
    row_grads = pull_term - hinge_rate * centered + cov_scale * (products - centered * spread[:, None, :])
    row_grads = row_grads.astype(jnp.bfloat16)
    across = (((0,), (0,)), ((), ()))
    left_term = lax.dot_general(hidden_a, row_grads[0], across, preferred_element_type=jnp.float32)
    right_term = lax.dot_general(hidden_b, row_grads[1], across, preferred_element_type=jnp.float32)
    return left_term + right_term
```

```python
import jax
import jax.numpy as jnp
from jax import lax
from jax.sharding import Mesh
from jax.sharding import PartitionSpec as P

epsilon = 0.0001


def shifted(array, axis, step):
    size = lax.axis_size(axis)
    return lax.ppermute(array, axis, [(i, (i + step) % size) for i in range(size)])


def part(array, index, count, dim):
    size = array.shape[dim] // count
    return lax.dynamic_slice_in_dim(array, index * size, size, dim)


def rows_for_features(hidden_a, hidden_b):
    place, count = lax.axis_index("crop"), lax.axis_size("crop")
    rows, feats = hidden_a.shape
    chips = lax.axis_size("x")
    both = jnp.stack(
        [h.reshape(chips, rows // chips, feats) for h in (hidden_a, hidden_b)], axis=1
    )
    whole = jnp.zeros((chips, 2, count, rows // chips, feats // count), both.dtype)
    for step in range(count):
        piece = part(both, (place + step) % count, count, 3)
        if step:
            piece = shifted(piece, "crop", step)
        whole = lax.dynamic_update_slice(
            whole, piece[:, :, None], (0, 0, (place - step) % count, 0, 0)
        )
    return whole


def body(hidden_a, hidden_b, weight):
    view, chip, plane = lax.axis_index("core"), lax.axis_index("x"), lax.axis_index("tensor")
    chips, planes = lax.axis_size("x"), lax.axis_size("tensor")
    total_rows = hidden_a.shape[0] * lax.axis_size("crop")
    first = view == 0
    other = jnp.where(first, hidden_b, hidden_a)
    own = jnp.where(first, hidden_a, hidden_b)
    passed = jnp.dot(other, weight, preferred_element_type=jnp.float32).astype(jnp.bfloat16)
    passed = shifted(passed, "core", 1)
    partial = jnp.dot(own, weight, preferred_element_type=jnp.float32) + passed.astype(jnp.float32)
    features = rows_for_features(hidden_a, hidden_b)
    total = part(partial, chip, chips, 0)
    for step in range(1, chips):
        sent = part(partial, (chip + step) % chips, chips, 0).astype(jnp.bfloat16)
        total = total + shifted(sent, "x", step).astype(jnp.float32)
    mine_low = total.astype(jnp.bfloat16)
    mine = mine_low.astype(jnp.float32)
    theirs = shifted(mine_low, "core", 1).astype(jnp.float32)

    everyone = lax.all_gather(mine_low, ("x", "crop"), axis=0, tiled=True).astype(jnp.float32)
    col_means = jnp.mean(everyone, axis=0)
    centered_all = everyone - col_means
    spread = jnp.sum(centered_all * centered_all, axis=0)
    deviation = jnp.sqrt(spread / (total_rows - 1.0) + epsilon)
    rounded_all = centered_all.astype(jnp.bfloat16)
    centered = mine - col_means
    rounded = centered.astype(jnp.bfloat16)

    gram = jnp.einsum("rf,bf->rb", rounded, rounded_all, preferred_element_type=jnp.float32)
    gram_sum = part(gram, plane, planes, 0)
    for step in range(1, planes):
        sent = part(gram, (plane + step) % planes, planes, 0).astype(jnp.bfloat16)
        gram_sum = gram_sum + shifted(sent, "tensor", step).astype(jnp.float32)
    gram_low = lax.all_gather(gram_sum.astype(jnp.bfloat16), "tensor", axis=0, tiled=True)
    products = jnp.dot(gram_low, rounded_all, preferred_element_type=jnp.float32)

    hinge_rate = jnp.where(deviation < 1.0, 25.0 / ((total_rows - 1.0) * deviation), 0.0)
    cov_scale = 4.0 / (total_rows - 1.0) ** 2
    row_grads = (
        (mine - theirs) * (50.0 / total_rows)
        - hinge_rate * centered
        + cov_scale * (products - centered * spread)
    ).astype(jnp.bfloat16)
    grads = lax.all_gather(row_grads, ("x", "core", "crop"), axis=0)
    grads = grads.reshape(-1, grads.shape[-1])
    features = features.reshape(-1, features.shape[-1])
    return lax.dot_general(
        features, grads, (((0,), (0,)), ((), ())), preferred_element_type=jnp.float32
    )


def solution(mesh):
    cores = 2
    split = Mesh(
        mesh.devices.reshape(mesh.shape["dp"] // cores, cores, *mesh.devices.shape[1:]),
        ("x", "core", "crop", "tensor"),
    )
    chips = ("x", "core")
    placed = (P("crop", chips), P("crop", chips), P(chips, "tensor"))
    return jax.shard_map(
        body,
        mesh=split,
        in_specs=placed,
        out_specs=P(("x", "core", "crop"), "tensor"),
        check_vma=False,
    )
```

```python
import jax
import jax.numpy as jnp
from jax import lax
from jax.sharding import Mesh
from jax.sharding import PartitionSpec as P

epsilon = 0.0001
others = (1, -1, 2)


def shifted(array, axis, step):
    size = lax.axis_size(axis)
    return lax.ppermute(array, axis, [(i, (i + step) % size) for i in range(size)])


def part(array, index, count, dim):
    size = array.shape[dim] // count
    return lax.dynamic_slice_in_dim(array, (index % count) * size, size, dim)


def summed(pieces, axis):
    total = pieces(0)
    for step in others:
        sent = pieces(step).astype(jnp.bfloat16)
        total = total + shifted(sent, axis, step).astype(jnp.float32)
    return total


def spread_over(array, axis):
    return [array] + [shifted(array, axis, step) for step in others]


def in_place(pieces, axis, dim):
    place = lax.axis_index(axis)
    size = pieces[0].shape[dim]
    shape = list(pieces[0].shape)
    shape[dim] = 4 * size
    whole = jnp.zeros(shape, pieces[0].dtype)
    for step, piece in zip((0, *others), pieces):
        whole = lax.dynamic_update_slice_in_dim(whole, piece, (place - step) % 4 * size, dim)
    return whole


def from_ring(whole, axis, dim):
    half = whole.shape[dim] // 2
    up, down = shifted(whole, axis, 1), shifted(whole, axis, -1)
    far = (
        shifted(lax.slice_in_dim(up, 0, half, axis=dim), axis, 1),
        shifted(lax.slice_in_dim(down, half, 2 * half, axis=dim), axis, -1),
    )
    return up, down, far


def matmul_rows(left, right):
    return lax.dot_general(left, right, (((0,), (0,)), ((), ())), preferred_element_type=jnp.float32)


def rows_for_features(hidden_a, hidden_b):
    place, count = lax.axis_index("crop"), lax.axis_size("crop")
    both = jnp.stack([hidden_a, hidden_b])
    return [part(both, place, count, 2)] + [
        shifted(part(both, place + step, count, 2), "crop", step) for step in others
    ]


def body(hidden_a, hidden_b, weight):
    view, chip, plane = lax.axis_index("core"), lax.axis_index("x"), lax.axis_index("tensor")
    total_rows = hidden_a.shape[0] * lax.axis_size("crop")
    first = view == 0
    passed = jnp.dot(
        jnp.where(first, hidden_b, hidden_a), weight, preferred_element_type=jnp.float32
    ).astype(jnp.bfloat16)
    own_part = jnp.dot(
        jnp.where(first, hidden_a, hidden_b), weight, preferred_element_type=jnp.float32
    )
    passed, own_part = shifted(passed, "core", 1), lax.optimization_barrier(own_part)
    total = summed(
        lambda step: part(own_part, chip + step, 4, 1)
        + part(passed, chip + step, 4, 1).astype(jnp.float32),
        "x",
    )
    mine_low = total.astype(jnp.bfloat16)
    features = rows_for_features(hidden_a, hidden_b)
    mine_low, features = lax.optimization_barrier((mine_low, features))
    mine = mine_low.astype(jnp.float32)
    theirs = shifted(mine_low, "core", 1).astype(jnp.float32)

    everyone = jnp.concatenate(spread_over(mine_low, "crop")).astype(jnp.float32)
    col_means = jnp.mean(everyone, axis=0)
    centered_all = everyone - col_means
    spread = jnp.sum(centered_all * centered_all, axis=0)
    deviation = jnp.sqrt(spread / (total_rows - 1.0) + epsilon)
    rounded_all = centered_all.astype(jnp.bfloat16)
    centered = mine - col_means
    rounded = centered.astype(jnp.bfloat16)

    gram = jnp.einsum("rf,bf->rb", rounded, rounded_all, preferred_element_type=jnp.float32)
    half = gram.shape[0] // 2
    ways = (("x", chip, "tensor", gram[:half]), ("tensor", plane, "x", gram[half:]))
    sums = [summed(lambda step: part(g, at + step, 4, 0), axis) for axis, at, _, g in ways]
    sums = [
        summed(lambda step: s, then).astype(jnp.bfloat16) for s, (_, _, then, _) in zip(sums, ways)
    ]
    gram_low = jnp.concatenate(
        [in_place(spread_over(s, axis), axis, 0) for s, (axis, _, _, _) in zip(sums, ways)]
    )
    products = jnp.dot(gram_low, rounded_all, preferred_element_type=jnp.float32)

    hinge_rate = jnp.where(deviation < 1.0, 25.0 / ((total_rows - 1.0) * deviation), 0.0)
    cov_scale = 4.0 / (total_rows - 1.0) ** 2
    row_grads = (
        (mine - theirs) * (50.0 / total_rows)
        - hinge_rate * centered
        + cov_scale * (products - centered * spread)
    ).astype(jnp.bfloat16)

    features = jnp.stack(features, axis=1)
    own_view = jnp.where(first, features[0], features[1])
    other_view = jnp.where(first, features[1], features[0])
    wanted = jnp.concatenate([own_view, shifted(other_view, "core", 1)], axis=-1)
    near, far = wanted[:, :half], wanted[:, half:]
    flat = lambda array: array.reshape(-1, array.shape[-1])

    tall = jnp.concatenate(spread_over(row_grads[:half], "crop"))
    wide = jnp.concatenate(spread_over(row_grads[half:], "x"), axis=1)
    tall_up, tall_down, tall_far = from_ring(tall, "x", 0)
    wide_up, wide_down, wide_far = from_ring(wide, "crop", 0)
    near = flat(near)
    block = lambda array: matmul_rows(near, array)
    out = jnp.concatenate(
        [block(tall), block(tall_up), block(tall_down), block(jnp.concatenate(tall_far))], axis=1
    )
    out = out + matmul_rows(far[0], wide)
    out = out + matmul_rows(far[1], wide_up)
    out = out + matmul_rows(far[2], wide_down)
    out = out + matmul_rows(far[3], jnp.concatenate(wide_far))
    count = out.shape[0] // 2
    out = out[:count] + shifted(out[count:], "core", 1)
    return in_place(jnp.split(out, 4, axis=1), "x", 1)


def solution(mesh):
    cores = 2
    split = Mesh(
        mesh.devices.reshape(mesh.shape["dp"] // cores, cores, *mesh.devices.shape[1:]),
        ("x", "core", "crop", "tensor"),
    )
    chips = ("x", "core")
    placed = (P("crop", chips), P("crop", chips), P(chips, "tensor"))
    return jax.shard_map(
        body,
        mesh=split,
        in_specs=placed,
        out_specs=P(("x", "core", "crop"), "tensor"),
        check_vma=False,
    )
```

```python
import jax
import jax.numpy as jnp
from jax import lax
from jax.sharding import Mesh
from jax.sharding import PartitionSpec as P

epsilon = 0.0001
others = (1, -1, 2)


def shifted(array, axis, step):
    size = lax.axis_size(axis)
    return lax.ppermute(array, axis, [(i, (i + step) % size) for i in range(size)])


def part(array, index, count, dim):
    size = array.shape[dim] // count
    return lax.dynamic_slice_in_dim(array, (index & (count - 1)) * size, size, dim, allow_negative_indices=False)


def made(pieces):
    return pieces(0), [pieces(step).astype(jnp.bfloat16) for step in others]


def summed(pieces, axis):
    total, sent = pieces
    received = [shifted(piece, axis, step) for piece, step in zip(sent, others)]
    for piece in received:
        total = total + piece.astype(jnp.float32)
    return total


def spread_over(array, axis):
    return [array] + [shifted(array, axis, step) for step in others]


def in_place(pieces, axis, dim):
    place = lax.axis_index(axis)
    size = pieces[0].shape[dim]
    shape = list(pieces[0].shape)
    shape[dim] = 4 * size
    whole = jnp.zeros(shape, pieces[0].dtype)
    for step, piece in zip((0, *others), pieces):
        whole = lax.dynamic_update_slice_in_dim(whole, piece, ((place - step) & 3) * size, dim, allow_negative_indices=False)
    return whole


def from_ring(whole, axis, dim):
    half = whole.shape[dim] // 2
    up, down = shifted(whole, axis, 1), shifted(whole, axis, -1)
    far = (
        shifted(lax.slice_in_dim(up, 0, half, axis=dim), axis, 1),
        shifted(lax.slice_in_dim(down, half, 2 * half, axis=dim), axis, -1),
    )
    return up, down, far


def matmul_rows(left, right):
    return lax.dot_general(left, right, (((0,), (0,)), ((), ())), preferred_element_type=jnp.float32)


def rows_for_features(hidden_a, hidden_b):
    place, count = lax.axis_index("crop"), lax.axis_size("crop")
    both = jnp.stack([hidden_a, hidden_b])
    return [part(both, place, count, 2)] + [
        shifted(part(both, place + step, count, 2), "crop", step) for step in others
    ]


def body(hidden_a, hidden_b, weight):
    view, chip, plane = lax.axis_index("core"), lax.axis_index("x"), lax.axis_index("tensor")
    total_rows = hidden_a.shape[0] * lax.axis_size("crop")
    first = view == 0
    own_rows = jnp.where(first, hidden_a, hidden_b)
    other_rows = jnp.where(first, hidden_b, hidden_a)
    own_rows, other_rows = lax.optimization_barrier((own_rows, other_rows))
    passed = jnp.dot(other_rows, weight, preferred_element_type=jnp.float32).astype(jnp.bfloat16)
    own_part = jnp.dot(own_rows, weight, preferred_element_type=jnp.float32)
    passed, own_part = shifted(passed, "core", 1), lax.optimization_barrier(own_part)
    mine_low, everyone = [], []
    pieces = []
    for chunk in range(2):
        at = lambda step: 2 * ((chip + step) & 3) + chunk
        pieces.append(
            made(
                lambda step: part(own_part, at(step), 8, 1)
                + part(passed, at(step), 8, 1).astype(jnp.float32)
            )
        )
    pieces = lax.optimization_barrier(pieces)
    for chunk in range(2):
        total = summed(pieces[chunk], "x")
        mine_low.append(total.astype(jnp.bfloat16))
    for chunk in range(2):
        everyone.append(jnp.concatenate(spread_over(mine_low[chunk], "crop")))
    mine_low = jnp.concatenate(mine_low, axis=1)
    mine = mine_low.astype(jnp.float32)
    theirs = shifted(mine_low, "core", 1).astype(jnp.float32)

    gram, rounded_all, col_means, spread = 0.0, [], [], []
    rows = mine.shape[0]
    for chunk in everyone:
        chunk = chunk.astype(jnp.float32)
        col_means.append(jnp.mean(chunk, axis=0))
        centered = chunk - col_means[-1]
        spread.append(jnp.sum(centered * centered, axis=0))
        low = centered.astype(jnp.bfloat16)
        rounded_all.append(low)
        gram = gram + jnp.einsum("rf,bf->rb", low[:rows], low, preferred_element_type=jnp.float32)
    col_means, spread = jnp.concatenate(col_means), jnp.concatenate(spread)
    rounded_all = jnp.concatenate(rounded_all, axis=1)
    deviation = jnp.sqrt(spread / (total_rows - 1.0) + epsilon)
    centered = mine - col_means

    gram, hidden_a, hidden_b = lax.optimization_barrier((gram, hidden_a, hidden_b))
    features = rows_for_features(hidden_a, hidden_b)
    half = rows // 2
    ways = (("x", chip, "tensor", gram[:half]), ("tensor", plane, "x", gram[half:]))
    sums = [
        summed(made(lambda step: part(g, at + step, 4, 0)), axis)
        for axis, at, _, g in ways
    ]
    sums = [summed(made(lambda step: s), then).astype(jnp.bfloat16) for s, (_, _, then, _) in zip(sums, ways)]
    gram_low = jnp.concatenate(
        [in_place(spread_over(s, axis), axis, 0) for s, (axis, _, _, _) in zip(sums, ways)]
    )
    gram_low, features = lax.optimization_barrier((gram_low, features))
    products = jnp.dot(gram_low, rounded_all, preferred_element_type=jnp.float32)

    hinge_rate = jnp.where(deviation < 1.0, 25.0 / ((total_rows - 1.0) * deviation), 0.0)
    cov_scale = 4.0 / (total_rows - 1.0) ** 2
    row_grads = (
        (mine - theirs) * (50.0 / total_rows)
        - hinge_rate * centered
        + cov_scale * (products - centered * spread)
    ).astype(jnp.bfloat16)

    features = jnp.stack(features, axis=1)
    own_view = jnp.where(first, features[0], features[1])
    other_view = jnp.where(first, features[1], features[0])
    wanted = (shifted(other_view, "core", 1), own_view)

    tall = jnp.concatenate(spread_over(row_grads[:half], "crop"))
    wide = in_place(spread_over(row_grads[half:], "x"), "x", 1)
    tall_up, tall_down, tall_far = from_ring(tall, "x", 0)
    wide_up, wide_down, wide_far = from_ring(wide, "crop", 0)
    parts = []
    for rows_wanted in wanted:
        near, far = rows_wanted[:, :half], rows_wanted[:, half:]
        near = near.reshape(-1, near.shape[-1])
        block = lambda array: matmul_rows(near, array)
        out = matmul_rows(far[0], wide) + matmul_rows(far[1], wide_up)
        out = out + matmul_rows(far[2], wide_down)
        talls = (tall, tall_up, tall_down, jnp.concatenate(tall_far))
        out = out + in_place([block(array) for array in talls], "x", 1)
        parts.append(out + matmul_rows(far[3], jnp.concatenate(wide_far)))
    return shifted(parts[0], "core", 1) + parts[1]


def solution(mesh):
    cores = 2
    split = Mesh(
        mesh.devices.reshape(mesh.shape["dp"] // cores, cores, *mesh.devices.shape[1:]),
        ("x", "core", "crop", "tensor"),
    )
    chips = ("x", "core")
    placed = (P("crop", chips), P("crop", chips), P(chips, "tensor"))
    return jax.shard_map(
        body,
        mesh=split,
        in_specs=placed,
        out_specs=P(("x", "core", "crop"), "tensor"),
        check_vma=False,
    )
```

```python
import jax
import jax.numpy as jnp
from jax import lax
from jax.sharding import Mesh
from jax.sharding import PartitionSpec as P

epsilon = 0.0001
others = (1, -1, 2)


def shifted(array, axis, step):
    size = lax.axis_size(axis)
    return lax.ppermute(array, axis, [(i, (i + step) % size) for i in range(size)])


def part(array, index, count, dim):
    size = array.shape[dim] // count
    return lax.dynamic_slice_in_dim(array, (index & (count - 1)) * size, size, dim, allow_negative_indices=False)


def made(pieces):
    return pieces(0), [pieces(step).astype(jnp.bfloat16) for step in others]


def summed(pieces, axis):
    total, sent = pieces
    received = [shifted(piece, axis, step) for piece, step in zip(sent, others)]
    for piece in received:
        total = total + piece.astype(jnp.float32)
    return total


def spread_over(array, axis):
    return [array] + [shifted(array, axis, step) for step in others]


def in_place(pieces, place, dim):
    size = pieces[0].shape[dim]
    shape = list(pieces[0].shape)
    shape[dim] = 4 * size
    whole = jnp.zeros(shape, pieces[0].dtype)
    for step, piece in zip((0, *others), pieces):
        whole = lax.dynamic_update_slice_in_dim(whole, piece, ((place - step) & 3) * size, dim, allow_negative_indices=False)
    return whole


def from_ring(whole, axis, dim):
    half = whole.shape[dim] // 2
    up, down = shifted(whole, axis, 1), shifted(whole, axis, -1)
    far = (
        shifted(lax.slice_in_dim(up, 0, half, axis=dim), axis, 1),
        shifted(lax.slice_in_dim(down, half, 2 * half, axis=dim), axis, -1),
    )
    return up, down, far


def matmul_rows(left, right):
    return lax.dot_general(left, right, (((0,), (0,)), ((), ())), preferred_element_type=jnp.float32)


def rows_for_features(hidden_a, hidden_b):
    place, count = lax.axis_index("crop"), lax.axis_size("crop")
    both = jnp.stack([hidden_a, hidden_b])
    return [part(both, place, count, 2)] + [
        shifted(part(both, place + step, count, 2), "crop", step) for step in others
    ]


def body(hidden_a, hidden_b, weight):
    view, chip, plane = lax.axis_index("core"), lax.axis_index("x"), lax.axis_index("tensor")
    total_rows = hidden_a.shape[0] * lax.axis_size("crop")
    first = view == 0
    own_rows = jnp.where(first, hidden_a, hidden_b)
    other_rows = jnp.where(first, hidden_b, hidden_a)
    own_rows, other_rows = lax.optimization_barrier((own_rows, other_rows))
    chunks, half = 2, hidden_a.shape[0] // 2
    project = lambda rows: jnp.dot(rows, weight, preferred_element_type=jnp.float32)
    pieces = []
    for chunk in range(chunks):
        rows = slice(chunk * half, (chunk + 1) * half)
        passed = shifted(project(other_rows[rows]).astype(jnp.bfloat16), "core", 1)
        own_part = lax.optimization_barrier(project(own_rows[rows]))
        made_here = made(
            lambda step: part(own_part, chip + step, 4, 1)
            + part(passed, chip + step, 4, 1).astype(jnp.float32)
        )
        made_here, own_rows, other_rows = lax.optimization_barrier(
            (made_here, own_rows, other_rows)
        )
        pieces.append(made_here)
    mine_low, everyone = [], []
    for chunk in range(chunks):
        total = summed(pieces[chunk], "x")
        mine_low.append(lax.optimization_barrier(total.astype(jnp.bfloat16)))
    for chunk in range(chunks):
        everyone += spread_over(mine_low[chunk], "crop")
    mine_low = jnp.concatenate(mine_low)
    mine = mine_low.astype(jnp.float32)
    theirs = shifted(mine_low, "core", 1).astype(jnp.float32)

    everyone = jnp.concatenate(everyone).astype(jnp.float32)
    col_means = jnp.mean(everyone, axis=0)
    centered_all = everyone - col_means
    spread = jnp.sum(centered_all * centered_all, axis=0)
    rounded_all = centered_all.astype(jnp.bfloat16)
    deviation = jnp.sqrt(spread / (total_rows - 1.0) + epsilon)
    centered = mine - col_means
    gram = jnp.einsum(
        "rf,bf->rb", centered.astype(jnp.bfloat16), rounded_all, preferred_element_type=jnp.float32
    )

    gram, hidden_a, hidden_b = lax.optimization_barrier((gram, hidden_a, hidden_b))
    features = rows_for_features(hidden_a, hidden_b)
    ways = (("x", chip, "tensor", gram[:half]), ("tensor", plane, "x", gram[half:]))
    sums = [
        summed(made(lambda step: part(g, at + step, 4, 0)), axis)
        for axis, at, _, g in ways
    ]
    sums = [summed(made(lambda step: s), then).astype(jnp.bfloat16) for s, (_, _, then, _) in zip(sums, ways)]
    gram_low = []
    for s, (axis, at, _, _) in zip(sums, ways):
        gram_low.append(in_place(spread_over(s, axis), at, 0))
    gram_low, features = lax.optimization_barrier((jnp.concatenate(gram_low), features))
    products = jnp.dot(gram_low, rounded_all, preferred_element_type=jnp.float32)

    hinge_rate = jnp.where(deviation < 1.0, 25.0 / ((total_rows - 1.0) * deviation), 0.0)
    cov_scale = 4.0 / (total_rows - 1.0) ** 2
    row_grads = (
        (mine - theirs) * (50.0 / total_rows)
        - hinge_rate * centered
        + cov_scale * (products - centered * spread)
    ).astype(jnp.bfloat16)

    features = jnp.stack(features, axis=1)
    own_view = jnp.where(first, features[0], features[1])
    other_view = jnp.where(first, features[1], features[0])
    wanted = (shifted(other_view, "core", 1), own_view)

    tall = jnp.concatenate(spread_over(row_grads[:half], "crop"))
    wide = in_place(spread_over(row_grads[half:], "x"), chip, 1)
    tall_up, tall_down, tall_far = from_ring(tall, "x", 0)
    wide_up, wide_down, wide_far = from_ring(wide, "crop", 0)
    parts = []
    for rows_wanted in wanted:
        near, far = rows_wanted[:, :half], rows_wanted[:, half:]
        near = near.reshape(-1, near.shape[-1])
        block = lambda array: matmul_rows(near, array)
        out = matmul_rows(far[0], wide) + matmul_rows(far[1], wide_up)
        out = out + matmul_rows(far[2], wide_down)
        talls = (tall, tall_up, tall_down, jnp.concatenate(tall_far))
        out = out + in_place([block(array) for array in talls], chip, 1)
        parts.append(out + matmul_rows(far[3], jnp.concatenate(wide_far)))
    return shifted(parts[0], "core", 1) + parts[1]


def solution(mesh):
    cores = 2
    split = Mesh(
        mesh.devices.reshape(mesh.shape["dp"] // cores, cores, *mesh.devices.shape[1:]),
        ("x", "core", "crop", "tensor"),
    )
    chips = ("x", "core")
    placed = (P("crop", chips), P("crop", chips), P(chips, "tensor"))
    return jax.shard_map(
        body,
        mesh=split,
        in_specs=placed,
        out_specs=P(("x", "core", "crop"), "tensor"),
        check_vma=False,
    )
```

```python
import jax
import jax.numpy as jnp
from jax import lax
from jax.sharding import Mesh
from jax.sharding import PartitionSpec as P

epsilon = 0.0001
others = (1, -1, 2)


def shifted(array, axis, step):
    size = lax.axis_size(axis)
    return lax.ppermute(array, axis, [(i, (i + step) % size) for i in range(size)])


def part(array, index, count, dim):
    size = array.shape[dim] // count
    return lax.dynamic_slice_in_dim(array, (index & (count - 1)) * size, size, dim, allow_negative_indices=False)


def made(pieces):
    return pieces(0), [pieces(step).astype(jnp.bfloat16) for step in others]


def summed(pieces, axis):
    total, sent = pieces
    received = [shifted(piece, axis, step) for piece, step in zip(sent, others)]
    for piece in received:
        total = total + piece.astype(jnp.float32)
    return total


def spread_over(array, axis):
    return [array] + [shifted(array, axis, step) for step in others]


def in_place(pieces, place, dim):
    size = pieces[0].shape[dim]
    shape = list(pieces[0].shape)
    shape[dim] = 4 * size
    whole = jnp.zeros(shape, pieces[0].dtype)
    for step, piece in zip((0, *others), pieces):
        whole = lax.dynamic_update_slice_in_dim(whole, piece, ((place - step) & 3) * size, dim, allow_negative_indices=False)
    return whole


def from_ring(whole, axis, dim, early=None):
    half = whole.shape[dim] // 2
    up, down = shifted(whole, axis, 1), shifted(whole, axis, -1)
    if early is not None:
        up, down = (jnp.concatenate(pair, axis=dim) for pair in zip(early, (up, down)))
        half = up.shape[dim] // 2
    far = (
        shifted(lax.slice_in_dim(up, 0, half, axis=dim), axis, 1),
        shifted(lax.slice_in_dim(down, half, 2 * half, axis=dim), axis, -1),
    )
    return up, down, far


def matmul_rows(left, right):
    return lax.dot_general(left, right, (((0,), (0,)), ((), ())), preferred_element_type=jnp.float32)


def rows_for_features(hidden_a, hidden_b):
    place, count = lax.axis_index("crop"), lax.axis_size("crop")
    both = jnp.stack([hidden_a, hidden_b])
    return [part(both, place, count, 2)] + [
        shifted(part(both, place + step, count, 2), "crop", step) for step in others
    ]


def body(hidden_a, hidden_b, weight):
    view, chip, plane = lax.axis_index("core"), lax.axis_index("x"), lax.axis_index("tensor")
    total_rows = hidden_a.shape[0] * lax.axis_size("crop")
    first = view == 0
    own_rows = jnp.where(first, hidden_a, hidden_b)
    other_rows = jnp.where(first, hidden_b, hidden_a)
    own_rows, other_rows = lax.optimization_barrier((own_rows, other_rows))
    chunks, half = 2, hidden_a.shape[0] // 2
    project = lambda rows: jnp.dot(rows, weight, preferred_element_type=jnp.float32)
    pieces = []
    for chunk in range(chunks):
        rows = slice(chunk * half, (chunk + 1) * half)
        passed = shifted(project(other_rows[rows]).astype(jnp.bfloat16), "core", 1)
        own_part = lax.optimization_barrier(project(own_rows[rows]))
        made_here = made(
            lambda step: part(own_part, chip + step, 4, 1)
            + part(passed, chip + step, 4, 1).astype(jnp.float32)
        )
        made_here, own_rows, other_rows = lax.optimization_barrier(
            (made_here, own_rows, other_rows)
        )
        pieces.append(made_here)
    mine_low, everyone = [], []
    for chunk in range(chunks):
        total = summed(pieces[chunk], "x")
        mine_low.append(lax.optimization_barrier(total.astype(jnp.bfloat16)))
    for chunk in range(chunks):
        everyone += spread_over(mine_low[chunk], "crop")
    mine_low = jnp.concatenate(mine_low)
    mine = mine_low.astype(jnp.float32)
    theirs = shifted(mine_low, "core", 1).astype(jnp.float32)

    everyone = jnp.concatenate(everyone).astype(jnp.float32)
    col_means = jnp.mean(everyone, axis=0)
    centered_all = everyone - col_means
    spread = jnp.sum(centered_all * centered_all, axis=0)
    rounded_all = centered_all.astype(jnp.bfloat16)
    deviation = jnp.sqrt(spread / (total_rows - 1.0) + epsilon)
    centered = mine - col_means
    gram = jnp.einsum(
        "rf,bf->rb", centered.astype(jnp.bfloat16), rounded_all, preferred_element_type=jnp.float32
    )

    gram, hidden_a, hidden_b = lax.optimization_barrier((gram, hidden_a, hidden_b))
    features = rows_for_features(hidden_a, hidden_b)
    ways = (("x", chip, "tensor", gram[:half]), ("tensor", plane, "x", gram[half:]))
    sums = [
        summed(made(lambda step: part(g, at + step, 4, 0)), axis)
        for axis, at, _, g in ways
    ]
    sums = [summed(made(lambda step: s), then).astype(jnp.bfloat16) for s, (_, _, then, _) in zip(sums, ways)]
    hinge_rate = jnp.where(deviation < 1.0, 25.0 / ((total_rows - 1.0) * deviation), 0.0)
    cov_scale = 4.0 / (total_rows - 1.0) ** 2
    row_grads = []
    for group, (s, (axis, at, _, _)) in enumerate(zip(sums, ways)):
        gram_low = in_place(spread_over(s, axis), at, 0)
        rows = slice(group * half, (group + 1) * half)
        products = jnp.dot(gram_low, rounded_all, preferred_element_type=jnp.float32)
        row_grads.append(
            lax.optimization_barrier(
                (
                    (mine[rows] - theirs[rows]) * (50.0 / total_rows)
                    - hinge_rate * centered[rows]
                    + cov_scale * (products - centered[rows] * spread)
                ).astype(jnp.bfloat16)
            )
        )

    row_grads[1], features = lax.optimization_barrier((row_grads[1], features))
    features = jnp.stack(features, axis=1)
    own_view = jnp.where(first, features[0], features[1])
    other_view = jnp.where(first, features[1], features[0])
    wanted = (shifted(other_view, "core", 1), own_view)

    talls = spread_over(row_grads[1], "crop")
    early = [shifted(row_grads[1], "x", step) for step in (1, -1)]
    wide = in_place(spread_over(row_grads[0], "x"), chip, 1)
    tall_up, tall_down, tall_far = from_ring(jnp.concatenate(talls[1:]), "x", 0, early)
    tall = jnp.concatenate(talls)
    wide_up, wide_down, wide_far = from_ring(wide, "crop", 0)
    parts = []
    for rows_wanted in wanted:
        far, near = rows_wanted[:, :half], rows_wanted[:, half:]
        near = near.reshape(-1, near.shape[-1])
        block = lambda array: matmul_rows(near, array)
        out = matmul_rows(far[0], wide) + matmul_rows(far[1], wide_up)
        out = out + matmul_rows(far[2], wide_down)
        talls = (tall, tall_up, tall_down, jnp.concatenate(tall_far))
        out = out + in_place([block(array) for array in talls], chip, 1)
        parts.append(out + matmul_rows(far[3], jnp.concatenate(wide_far)))
    return shifted(parts[0], "core", 1) + parts[1]


def solution(mesh):
    cores = 2
    split = Mesh(
        mesh.devices.reshape(mesh.shape["dp"] // cores, cores, *mesh.devices.shape[1:]),
        ("x", "core", "crop", "tensor"),
    )
    chips = ("x", "core")
    placed = (P("crop", chips), P("crop", chips), P(chips, "tensor"))
    return jax.shard_map(
        body,
        mesh=split,
        in_specs=placed,
        out_specs=P(("x", "core", "crop"), "tensor"),
        check_vma=False,
    )
```

```python
import jax
import jax.numpy as jnp
from jax import lax
from jax.experimental import pallas as pl
from jax.sharding import Mesh
from jax.sharding import PartitionSpec as P

epsilon = 0.0001
others = (1, -1, 2)


def shifted(array, axis, step):
    size = lax.axis_size(axis)
    return lax.ppermute(array, axis, [(i, (i + step) % size) for i in range(size)])


def part(array, index, count, dim):
    size = array.shape[dim] // count
    return lax.dynamic_slice_in_dim(array, (index & (count - 1)) * size, size, dim, allow_negative_indices=False)


def made(pieces):
    return pieces(0), [pieces(step).astype(jnp.bfloat16) for step in others]


def summed(pieces, axis):
    total, sent = pieces
    received = [shifted(piece, axis, step) for piece, step in zip(sent, others)]
    for piece in received:
        total = total + piece.astype(jnp.float32)
    return total


def spread_over(array, axis):
    return [array] + [shifted(array, axis, step) for step in others]


def in_place(pieces, place, dim, whole=None):
    size = pieces[0].shape[dim]
    shape = list(pieces[0].shape)
    shape[dim] = 4 * size
    whole = jnp.zeros(shape, pieces[0].dtype) if whole is None else whole
    for step, piece in zip((0, *others), pieces):
        whole = lax.dynamic_update_slice_in_dim(whole, piece, ((place - step) & 3) * size, dim, allow_negative_indices=False)
    return whole


def from_ring(whole, axis, dim, early=None):
    half = whole.shape[dim] // 2
    up, down = shifted(whole, axis, 1), shifted(whole, axis, -1)
    if early is not None:
        up, down = (jnp.concatenate(pair, axis=dim) for pair in zip(early, (up, down)))
        half = up.shape[dim] // 2
    far = (
        shifted(lax.slice_in_dim(up, 0, half, axis=dim), axis, 1),
        shifted(lax.slice_in_dim(down, half, 2 * half, axis=dim), axis, -1),
    )
    return up, down, far


def matmul_rows(left, right):
    return lax.dot_general(left, right, (((0,), (0,)), ((), ())), preferred_element_type=jnp.float32)


def projected(all_rows, weight, chunk, chunks):
    rows, inner = all_rows.shape[0] // chunks, all_rows.shape[1]
    outer, tile = weight.shape[1], 256

    def kernel(rows_ref, weight_ref, out_ref):
        out_ref[...] = jnp.dot(
            rows_ref[...], weight_ref[...], preferred_element_type=jnp.float32
        )

    return pl.pallas_call(
        kernel,
        grid=(outer // tile,),
        in_specs=[
            pl.BlockSpec((rows, inner), lambda i: (chunk, 0)),
            pl.BlockSpec((inner, tile), lambda i: (0, i)),
        ],
        out_specs=pl.BlockSpec((rows, tile), lambda i: (0, i)),
        out_shape=jax.ShapeDtypeStruct((rows, outer), jnp.float32),
        cost_estimate=pl.CostEstimate(
            flops=2 * rows * inner * outer,
            transcendentals=0,
            bytes_accessed=2 * rows * inner + 2 * inner * outer + 4 * rows * outer,
        ),
        name="projected",
    )(all_rows, weight)


def rows_for_features(hidden_a, hidden_b):
    place, count = lax.axis_index("crop"), lax.axis_size("crop")
    both = jnp.stack([hidden_a, hidden_b])
    return [part(both, place, count, 2)] + [
        shifted(part(both, place + step, count, 2), "crop", step) for step in others
    ]


def body(hidden_a, hidden_b, weight):
    view, chip, plane = lax.axis_index("core"), lax.axis_index("x"), lax.axis_index("tensor")
    total_rows = hidden_a.shape[0] * lax.axis_size("crop")
    first = view == 0
    own_rows = jnp.where(first, hidden_a, hidden_b)
    other_rows = jnp.where(first, hidden_b, hidden_a)
    own_rows, other_rows = lax.optimization_barrier((own_rows, other_rows))
    chunks, half = 2, hidden_a.shape[0] // 2
    project = lambda rows: jnp.dot(rows, weight, preferred_element_type=jnp.float32)
    pieces, passed = [], []
    for chunk in range(chunks):
        rows = slice(chunk * half, (chunk + 1) * half)
        passed.append(shifted(project(other_rows[rows]).astype(jnp.bfloat16), "core", 1))
        if chunk == 0:
            own_part = project(own_rows[rows])
            own_part, other_rows = lax.optimization_barrier((own_part, other_rows))
    for chunk in range(chunks):
        if chunk:
            own_part = projected(own_rows, weight, chunk, chunks)
        made_here = made(
            lambda step: part(own_part, chip + step, 4, 1)
            + part(passed[chunk], chip + step, 4, 1).astype(jnp.float32)
        )
        made_here, own_rows = lax.optimization_barrier((made_here, own_rows))
        pieces.append(made_here)
    mine_low, everyone = [], []
    for chunk in range(chunks):
        total = summed(pieces[chunk], "x")
        mine_low.append(lax.optimization_barrier(total.astype(jnp.bfloat16)))
    for chunk in range(chunks):
        everyone += spread_over(mine_low[chunk], "crop")
    mine_low = jnp.concatenate(mine_low)
    mine = mine_low.astype(jnp.float32)
    theirs = shifted(mine_low, "core", 1).astype(jnp.float32)

    everyone = jnp.concatenate(everyone).astype(jnp.float32)
    col_means = jnp.mean(everyone, axis=0)
    centered_all = everyone - col_means
    spread = jnp.sum(centered_all * centered_all, axis=0)
    rounded_all = centered_all.astype(jnp.bfloat16)
    deviation = jnp.sqrt(spread / (total_rows - 1.0) + epsilon)
    centered = mine - col_means
    gram = jnp.einsum(
        "rf,bf->rb", centered.astype(jnp.bfloat16), rounded_all, preferred_element_type=jnp.float32
    )

    gram, hidden_a, hidden_b = lax.optimization_barrier((gram, hidden_a, hidden_b))
    features = rows_for_features(hidden_a, hidden_b)
    ways = (("x", chip, "tensor", gram[:half]), ("tensor", plane, "x", gram[half:]))
    sums = [
        summed(made(lambda step: part(g, at + step, 4, 0)), axis)
        for axis, at, _, g in ways
    ]
    sums = [summed(made(lambda step: s), then).astype(jnp.bfloat16) for s, (_, _, then, _) in zip(sums, ways)]
    hinge_rate = jnp.where(deviation < 1.0, 25.0 / ((total_rows - 1.0) * deviation), 0.0)
    cov_scale = 4.0 / (total_rows - 1.0) ** 2
    row_grads, old_gram = [], None
    for group, (s, (axis, at, _, _)) in enumerate(zip(sums, ways)):
        gram_low = in_place(spread_over(s, axis), at, 0)
        old_gram = old_gram if group else gram_low
        rows = slice(group * half, (group + 1) * half)
        products = jnp.dot(gram_low, rounded_all, preferred_element_type=jnp.float32)
        row_grads.append(
            lax.optimization_barrier(
                (
                    (mine[rows] - theirs[rows]) * (50.0 / total_rows)
                    - (hinge_rate + cov_scale * spread) * centered[rows]
                    + cov_scale * products
                ).astype(jnp.bfloat16)
            )
        )

    row_grads[1], features = lax.optimization_barrier((row_grads[1], features))
    own_view = jnp.stack([jnp.where(first, f[0], f[1]) for f in features])
    other_view = jnp.stack([jnp.where(first, f[1], f[0]) for f in features])
    wanted = (shifted(other_view, "core", 1), own_view)

    talls = spread_over(row_grads[1], "crop")
    early = [shifted(row_grads[1], "x", step) for step in (1, -1)]
    wide = in_place(spread_over(row_grads[0], "x"), chip, 1, old_gram)
    tall_up, tall_down, tall_far = from_ring(jnp.concatenate(talls[1:]), "x", 0, early)
    tall = jnp.concatenate(talls)
    wide_up, wide_down, wide_far = from_ring(wide, "crop", 0)
    parts = []
    for rows_wanted in wanted:
        far, near = rows_wanted[:, :half], rows_wanted[:, half:]
        near = near.reshape(-1, near.shape[-1])
        block = lambda array: matmul_rows(near, array)
        out = matmul_rows(far[0], wide) + matmul_rows(far[1], wide_up)
        out = out + matmul_rows(far[2], wide_down)
        talls = (tall, tall_up, tall_down, jnp.concatenate(tall_far))
        out = out + in_place([block(array) for array in talls], chip, 1)
        parts.append(out + matmul_rows(far[3], jnp.concatenate(wide_far)))
    return shifted(parts[0], "core", 1) + parts[1]


def solution(mesh):
    cores = 2
    split = Mesh(
        mesh.devices.reshape(mesh.shape["dp"] // cores, cores, *mesh.devices.shape[1:]),
        ("x", "core", "crop", "tensor"),
    )
    chips = ("x", "core")
    placed = (P("crop", chips), P("crop", chips), P(chips, "tensor"))
    return jax.shard_map(
        body,
        mesh=split,
        in_specs=placed,
        out_specs=P(("x", "core", "crop"), "tensor"),
        check_vma=False,
    )
```

```python
import jax
import jax.numpy as jnp
from jax import lax
from jax.experimental import pallas as pl
from jax.sharding import Mesh
from jax.sharding import PartitionSpec as P

epsilon = 0.0001
others = (1, -1, 2)


def shifted(array, axis, step):
    size = lax.axis_size(axis)
    return lax.ppermute(array, axis, [(i, (i + step) % size) for i in range(size)])


def part(array, index, count, dim):
    size = array.shape[dim] // count
    return lax.dynamic_slice_in_dim(array, (index & (count - 1)) * size, size, dim, allow_negative_indices=False)


def made(pieces):
    return pieces(0), [pieces(step).astype(jnp.bfloat16) for step in others]


def summed(pieces, axis):
    total, sent = pieces
    received = [shifted(piece, axis, step) for piece, step in zip(sent, others)]
    for piece in received:
        total = total + piece.astype(jnp.float32)
    return total


def spread_over(array, axis):
    return [array] + [shifted(array, axis, step) for step in others]


def in_place(pieces, place, dim):
    size = pieces[0].shape[dim]
    shape = list(pieces[0].shape)
    shape[dim] = 4 * size
    whole = jnp.zeros(shape, pieces[0].dtype)
    for step, piece in zip((0, *others), pieces):
        whole = lax.dynamic_update_slice_in_dim(whole, piece, ((place - step) & 3) * size, dim, allow_negative_indices=False)
    return whole


def from_ring(whole, axis, dim, early=None):
    half = whole.shape[dim] // 2
    up, down = shifted(whole, axis, 1), shifted(whole, axis, -1)
    if early is not None:
        up, down = (jnp.concatenate(pair, axis=dim) for pair in zip(early, (up, down)))
        half = up.shape[dim] // 2
    far = (
        shifted(lax.slice_in_dim(up, 0, half, axis=dim), axis, 1),
        shifted(lax.slice_in_dim(down, half, 2 * half, axis=dim), axis, -1),
    )
    return up, down, far


def matmul_rows(left, right):
    return lax.dot_general(left, right, (((0,), (0,)), ((), ())), preferred_element_type=jnp.float32)


def project_both(own_rows, other_rows, weight, chunk, chunks):
    rows, inner = own_rows.shape[0] // chunks, own_rows.shape[1]
    outer, tile = weight.shape[1], 512

    def kernel(own_ref, other_ref, weight_ref, sent_ref, out_ref):
        times = lambda ref: jnp.dot(ref[...], weight_ref[...], preferred_element_type=jnp.float32)
        sent_ref[...] = times(other_ref).astype(jnp.bfloat16)
        out_ref[...] = times(own_ref)

    row_block = pl.BlockSpec((rows, inner), lambda i: (chunk, 0))
    out_block = pl.BlockSpec((rows, tile), lambda i: (0, i))
    return pl.pallas_call(
        kernel,
        grid=(outer // tile,),
        in_specs=[row_block, row_block, pl.BlockSpec((inner, tile), lambda i: (0, i))],
        out_specs=[out_block, out_block],
        out_shape=[
            jax.ShapeDtypeStruct((rows, outer), jnp.bfloat16),
            jax.ShapeDtypeStruct((rows, outer), jnp.float32),
        ],
        cost_estimate=pl.CostEstimate(
            flops=4 * rows * inner * outer,
            transcendentals=0,
            bytes_accessed=4 * rows * inner + 2 * inner * outer + 6 * rows * outer,
        ),
        name="project",
    )(own_rows, other_rows, weight)


def rows_for_features(hidden_a, hidden_b):
    place, count = lax.axis_index("crop"), lax.axis_size("crop")
    both = jnp.stack([hidden_a, hidden_b])
    return [part(both, place, count, 2)] + [
        shifted(part(both, place + step, count, 2), "crop", step) for step in others
    ]


def body(hidden_a, hidden_b, weight):
    view, chip, plane = lax.axis_index("core"), lax.axis_index("x"), lax.axis_index("tensor")
    total_rows = hidden_a.shape[0] * lax.axis_size("crop")
    first = view == 0
    own_rows = jnp.where(first, hidden_a, hidden_b)
    other_rows = jnp.where(first, hidden_b, hidden_a)
    own_rows, other_rows = lax.optimization_barrier((own_rows, other_rows))
    chunks, half = 2, hidden_a.shape[0] // 2
    project = lambda rows: jnp.dot(rows, weight, preferred_element_type=jnp.float32)
    pieces = []
    for chunk in range(chunks):
        rows = slice(chunk * half, (chunk + 1) * half)
        if chunk == 0:
            passed = project(other_rows[rows]).astype(jnp.bfloat16)
            own_part = lax.optimization_barrier(project(own_rows[rows]))
        else:
            passed, own_part = project_both(own_rows, other_rows, weight, chunk, chunks)
        passed = shifted(passed, "core", 1)
        made_here = made(
            lambda step: part(own_part, chip + step, 4, 1)
            + part(passed, chip + step, 4, 1).astype(jnp.float32)
        )
        made_here, own_rows, other_rows = lax.optimization_barrier(
            (made_here, own_rows, other_rows)
        )
        pieces.append(made_here)
    mine_low, everyone = [], []
    for chunk in range(chunks):
        total = summed(pieces[chunk], "x")
        mine_low.append(lax.optimization_barrier(total.astype(jnp.bfloat16)))
    for chunk in range(chunks):
        everyone += spread_over(mine_low[chunk], "crop")
    mine_low = jnp.concatenate(mine_low)
    mine = mine_low.astype(jnp.float32)
    theirs = shifted(mine_low, "core", 1).astype(jnp.float32)

    everyone = jnp.concatenate(everyone).astype(jnp.float32)
    col_means = jnp.mean(everyone, axis=0)
    centered_all = everyone - col_means
    spread = jnp.sum(centered_all * centered_all, axis=0)
    rounded_all = centered_all.astype(jnp.bfloat16)
    deviation = jnp.sqrt(spread / (total_rows - 1.0) + epsilon)
    centered = mine - col_means
    gram = jnp.einsum(
        "rf,bf->rb", centered.astype(jnp.bfloat16), rounded_all, preferred_element_type=jnp.float32
    )

    gram, hidden_a, hidden_b = lax.optimization_barrier((gram, hidden_a, hidden_b))
    features = rows_for_features(hidden_a, hidden_b)
    ways = (("x", chip, "tensor", gram[:half]), ("tensor", plane, "x", gram[half:]))
    sums = [
        summed(made(lambda step: part(g, at + step, 4, 0)), axis)
        for axis, at, _, g in ways
    ]
    sums = [summed(made(lambda step: s), then).astype(jnp.bfloat16) for s, (_, _, then, _) in zip(sums, ways)]
    hinge_rate = jnp.where(deviation < 1.0, 25.0 / ((total_rows - 1.0) * deviation), 0.0)
    cov_scale = 4.0 / (total_rows - 1.0) ** 2
    row_grads = []
    for group, (s, (axis, at, _, _)) in enumerate(zip(sums, ways)):
        gram_low = in_place(spread_over(s, axis), at, 0)
        rows = slice(group * half, (group + 1) * half)
        products = jnp.dot(gram_low, rounded_all, preferred_element_type=jnp.float32)
        row_grads.append(
            lax.optimization_barrier(
                (
                    (mine[rows] - theirs[rows]) * (50.0 / total_rows)
                    - hinge_rate * centered[rows]
                    + cov_scale * (products - centered[rows] * spread)
                ).astype(jnp.bfloat16)
            )
        )

    row_grads[1], features = lax.optimization_barrier((row_grads[1], features))
    features = jnp.stack(features, axis=1)
    own_view = jnp.where(first, features[0], features[1])
    other_view = jnp.where(first, features[1], features[0])
    wanted = (shifted(other_view, "core", 1), own_view)

    talls = spread_over(row_grads[1], "crop")
    early = [shifted(row_grads[1], "x", step) for step in (1, -1)]
    wide = in_place(spread_over(row_grads[0], "x"), chip, 1)
    tall_up, tall_down, tall_far = from_ring(jnp.concatenate(talls[1:]), "x", 0, early)
    tall = jnp.concatenate(talls)
    wide_up, wide_down, wide_far = from_ring(wide, "crop", 0)
    parts = []
    for rows_wanted in wanted:
        far, near = rows_wanted[:, :half], rows_wanted[:, half:]
        near = near.reshape(-1, near.shape[-1])
        block = lambda array: matmul_rows(near, array)
        out = matmul_rows(far[0], wide) + matmul_rows(far[1], wide_up)
        out = out + matmul_rows(far[2], wide_down)
        talls = (tall, tall_up, tall_down, jnp.concatenate(tall_far))
        out = out + in_place([block(array) for array in talls], chip, 1)
        parts.append(out + matmul_rows(far[3], jnp.concatenate(wide_far)))
    return shifted(parts[0], "core", 1) + parts[1]


def solution(mesh):
    cores = 2
    split = Mesh(
        mesh.devices.reshape(mesh.shape["dp"] // cores, cores, *mesh.devices.shape[1:]),
        ("x", "core", "crop", "tensor"),
    )
    chips = ("x", "core")
    placed = (P("crop", chips), P("crop", chips), P(chips, "tensor"))
    return jax.shard_map(
        body,
        mesh=split,
        in_specs=placed,
        out_specs=P(("x", "core", "crop"), "tensor"),
        check_vma=False,
    )
```
